32 devices in a mesh: tm: 4 (over z), map: 8 (over y, x, core).
Axes of the slice: x: 2, y: 2, z: 4, core: 2. Of those that a mesh axis runs over, the one named last changes fastest.
Arguments:
- points: float32 [3, 32768, 128], P(None, ('tm', 'map')), may hold values from -6 to 6
- poses: float32 [6, 1024], P(None, ('tm', 'map')), may hold values from -1.5 to 1.5
- normal_angles: float32 [2, 8192], P(None, ('tm', 'map')), may hold values from -3.140625 to 3.140625
- voxel_ids: int32 [32768], P(('tm', 'map')), may hold values from -1 to 8191, as said below
- scan_ids: int32 [32768], P(('tm', 'map')), may hold values from 0 to 255
Outputs:
- hessian: float32 [36, 1024], P(None, ('tm', 'map'))
- gradient: float32 [6, 1024], P(None, ('tm', 'map'))
- plane_cost: float32 [8192], P(('tm', 'map'))
The draws below stay inside these ranges and needn't reach their ends.
Inputs may be any that keep to these rules, and one draw needn't show every extreme that they name: `voxel_ids`: -1 marks an empty slot. Otherwise the block at position s among the 1024 blocks of its device has its voxel among those of owner o = s // 32, that is, in [o * 256, (o + 1) * 256), where owners are devices in tm+map order. In every draw some owner gets a live block in every slot from every device.
All inputs are finite; a program needn't handle non-finite values.
Results may differ from the reference program's by a relative error of at most 0.0003.
Values sent between devices are 32-bit elements; how exact they have to be, the bound alone decides.
A program may use at most 128 MiB of HBM per device.

```python
import jax
import jax.numpy as jnp
from jax import lax

PTS = 128
CAP = 32
VOX_DEV = 256
BLK_DEV = 1024
BLOCKS = 32768
VOXELS = 8192
SCAN_ROW = 256
SCANS = 1024
N_MAP = 8
DEVICES = 32


def draw_voxel_ids(key, part):
    keys = jax.random.split(jax.random.fold_in(key, 71), 5)
    slot = jnp.arange(BLOCKS, dtype=jnp.int32)
    owner_of = slot % BLK_DEV // CAP
    hottest = jax.random.randint(keys[0], (), 0, DEVICES)
    level = jax.random.randint(keys[1], (DEVICES,), 3, 10)
    level = jnp.where(jnp.arange(DEVICES, dtype=jnp.int32) == hottest, 10, level)
    coin = jax.random.randint(keys[2], (BLOCKS,), 0, 10)
    first = jax.random.randint(keys[3], (BLOCKS,), 0, VOX_DEV)
    second = jax.random.randint(keys[4], (BLOCKS,), 0, VOX_DEV)
    picked = jnp.minimum(first, second)
    return jnp.where(coin < level[owner_of], owner_of * VOX_DEV + picked, -1).astype(jnp.int32)


def with_ends(result, stream_key, smallest, high):
    longest = result.shape.index(max(result.shape))
    spots = []
    for shift in (0, 1):
        where = [jax.random.randint(jax.random.fold_in(stream_key, axis), (), 0, length) for axis, length in enumerate(result.shape)]
        where[longest] = (where[longest] + shift) % result.shape[longest]
        spots.append(tuple(where))
    return result.at[spots[0]].set(smallest).at[spots[1]].set(high)


def block_scale(rng, extent, shards, smallest, top_value):
    def one(axis_at, parts):
        heights = jax.random.uniform(jax.random.fold_in(jax.random.fold_in(rng, 6), axis_at), (parts,), jnp.float32, smallest / len(shards), top_value / len(shards))
        return jnp.repeat(jnp.exp(heights), extent[axis_at] // parts).reshape((-1,) + (1,) * (len(extent) - axis_at - 1))

    factor_of = one(*shards[0])
    for cut in shards[1:]:
        factor_of = factor_of * one(*cut)
    return factor_of


def normal_values(stream_key, extent, spread, reach, shards=(), held_as=jnp.bfloat16):
    drawn = jax.random.normal(stream_key, extent, jnp.float32) * spread
    if len(shards) > 0:
        drawn = block_scale(stream_key, extent, shards, -0.22, 0.18) * drawn
    return jnp.clip(drawn, min=-reach, max=reach).astype(held_as)


def setup_inputs(seed: int = 0) -> dict:
    splits = jax.random.split(jax.random.key(seed), 6)
    return {
        "points": normal_values(splits[0], (3, BLOCKS, PTS), 1.0, 6.0, ((1, 32),), jnp.float32),
        "poses": jnp.clip(jax.random.uniform(splits[1], (6, SCANS), jnp.float32, -1.5, 1.5) * block_scale(splits[1], (6, SCANS), ((1, 32),), -0.4, 0.0), -1.5, 1.5),
        "normal_angles": jnp.clip(jax.random.uniform(splits[2], (2, VOXELS), jnp.float32, -3.140625, 3.140625), -3.140625, 3.140625),
        "voxel_ids": draw_voxel_ids(jax.random.fold_in(splits[5], 71), 0),
        "scan_ids": with_ends(jax.random.randint(splits[4], (BLOCKS,), 0, SCAN_ROW), jax.random.fold_in(splits[4], 1), 0, SCAN_ROW - 1).astype(jnp.int32),
    }


def rigid(angles):
    cos_x, sin_x = jnp.cos(angles[0]), jnp.sin(angles[0])
    cos_y, sin_y = jnp.cos(angles[1]), jnp.sin(angles[1])
    cos_z, sin_z = jnp.cos(angles[2]), jnp.sin(angles[2])
    return jnp.stack([
        cos_z * cos_y, cos_z * sin_y * sin_x - sin_z * cos_x, cos_z * sin_y * cos_x + sin_z * sin_x,
        sin_z * cos_y, sin_z * sin_y * sin_x + cos_z * cos_x, sin_z * sin_y * cos_x - cos_z * sin_x,
        -sin_y, cos_y * sin_x, cos_y * cos_x,
        angles[3], angles[4], angles[5]])


def transform(points, per_block):
    rows_out = []
    for axis_out in range(3):
        acc = per_block[9 + axis_out][:, None]
        for axis_in in range(3):
            acc = acc + per_block[3 * axis_out + axis_in][:, None] * points[axis_in]
        rows_out.append(acc)
    return jnp.stack(rows_out)


def moments_of(world_pts):
    first = jnp.sum(world_pts, axis=2)
    pairs = [(0, 0), (1, 1), (2, 2), (0, 1), (0, 2), (1, 2)]
    second = jnp.stack([jnp.sum(world_pts[i] * world_pts[j], axis=1) for i, j in pairs])
    return jnp.concatenate([first, second], axis=0)


def unit_normal(normal_angles):
    theta, phi = normal_angles[0], normal_angles[1]
    return jnp.stack([jnp.sin(theta) * jnp.cos(phi), jnp.sin(theta) * jnp.sin(phi), jnp.cos(theta)])


def block_terms(world_pts, normal, offset):
    cross = jnp.stack([
        world_pts[1] * normal[2][:, None] - world_pts[2] * normal[1][:, None],
        world_pts[2] * normal[0][:, None] - world_pts[0] * normal[2][:, None],
        world_pts[0] * normal[1][:, None] - world_pts[1] * normal[0][:, None]])
    normal_b = jnp.broadcast_to(normal[:, :, None], world_pts.shape)
    jacobian = jnp.concatenate([cross, normal_b], axis=0)
    resid = jnp.sum(world_pts * normal[:, :, None], axis=0) - offset[:, None]
    outer = jnp.einsum('ibp,jbp->ijb', jacobian, jacobian, precision=lax.Precision.HIGHEST)
    grad_b = jnp.einsum('ibp,bp->ib', jacobian, resid, precision=lax.Precision.HIGHEST)
    return jnp.concatenate([outer.reshape(36, -1), grad_b], axis=0)


def reference(points, poses, normal_angles, voxel_ids, scan_ids):
    pose_table = rigid(poses)
    block_index = jnp.arange(BLOCKS, dtype=jnp.int32)
    global_scan = (block_index // BLK_DEV // N_MAP) * SCAN_ROW + scan_ids
    is_live = voxel_ids >= 0

    def span_world(index):
        start = (index * BLK_DEV).astype(jnp.int32)
        pts = lax.dynamic_slice_in_dim(points, start, BLK_DEV, 1)
        scans = lax.dynamic_slice_in_dim(global_scan, start, BLK_DEV, 0)
        return transform(pts, pose_table[:, scans])

    def span_moments(index):
        start = (index * BLK_DEV).astype(jnp.int32)
        live_c = lax.dynamic_slice_in_dim(is_live, start, BLK_DEV, 0)
        return jnp.where(live_c[None, :], moments_of(span_world(index)), 0.0)

    moments = lax.map(span_moments, jnp.arange(DEVICES, dtype=jnp.int32))
    moments = jnp.transpose(moments, (0, 2, 1)).reshape(BLOCKS, 9)
    segment = jnp.where(is_live, voxel_ids, VOXELS)
    voxel_sums = jax.ops.segment_sum(moments, segment, num_segments=VOXELS + 1)[:VOXELS].T
    counts = jax.ops.segment_sum(is_live.astype(jnp.float32), segment, num_segments=VOXELS + 1)[:VOXELS] * PTS
    floor_count = jnp.maximum(counts, 1.0)
    normal = unit_normal(normal_angles)
    offset = jnp.sum(normal * voxel_sums[:3], axis=0) / floor_count
    quadric = (normal[0] ** 2 * voxel_sums[3] + normal[1] ** 2 * voxel_sums[4] + normal[2] ** 2 * voxel_sums[5]
               + 2.0 * (normal[0] * normal[1] * voxel_sums[6] + normal[0] * normal[2] * voxel_sums[7]
                        + normal[1] * normal[2] * voxel_sums[8]))
    plane_cost = quadric / floor_count - offset ** 2
    safe_ids = jnp.where(is_live, voxel_ids, 0)
    block_normal = jnp.where(is_live[None, :], normal[:, safe_ids], 0.0)
    block_offset = jnp.where(is_live, offset[safe_ids], 0.0)

    def span_terms(index):
        start = (index * BLK_DEV).astype(jnp.int32)
        norm_c = lax.dynamic_slice_in_dim(block_normal, start, BLK_DEV, 1)
        off_c = lax.dynamic_slice_in_dim(block_offset, start, BLK_DEV, 0)
        return block_terms(span_world(index), norm_c, off_c)

    terms = lax.map(span_terms, jnp.arange(DEVICES, dtype=jnp.int32))
    terms = jnp.transpose(terms, (0, 2, 1)).reshape(BLOCKS, 42)
    per_scan = jax.ops.segment_sum(terms, global_scan, num_segments=SCANS).T
    per_scan = per_scan * (SCANS / (BLOCKS * PTS))
    return per_scan[:36], per_scan[36:], plane_cost
```

```python
import functools

import jax
import jax.numpy as jnp
from jax import lax
from jax.experimental import pallas as pl
from jax.experimental.pallas import tpu as pltpu
from jax.sharding import PartitionSpec as P

LANES = 128
MESH = pl.DeviceIdType.MESH
PAIRS = [(0, 0), (1, 1), (2, 2), (0, 1), (0, 2), (1, 2)]
PAIR_ROW = {}
for _k, (_i, _j) in enumerate(PAIRS):
    PAIR_ROW[(_i, _j)] = _k
    PAIR_ROW[(_j, _i)] = _k


def parts_of(x):
    high = x.astype(jnp.bfloat16)
    rest = x - high.astype(jnp.float32)
    mid = rest.astype(jnp.bfloat16)
    low = (rest - mid.astype(jnp.float32)).astype(jnp.bfloat16)
    return jnp.concatenate([high, mid, low], axis=0)


def joined(y):
    rows = y.shape[0] // 3
    return y[:rows] + y[rows : 2 * rows] + y[2 * rows :]


def group_turn(pieces, out_group, group, lanes_per):
    total = None
    for a, piece in enumerate(pieces):
        shift = lax.rem((a - out_group) * lanes_per + LANES, LANES)
        if isinstance(out_group, int):
            shift = ((a - out_group) * lanes_per) % LANES
        moved = piece if isinstance(shift, int) and shift == 0 else pltpu.roll(piece, shift, 1)
        total = moved if total is None else jnp.where(group == a, moved, total)
    return total


def loop(count, body):
    if count <= 8:
        for i in range(count):
            body(i)
    else:
        def step(i, carry):
            body(i)
            return carry

        lax.fori_loop(0, count, step, 0)


def kernel(
    sizes,
    points,
    poses,
    angles,
    voxel_ids,
    scan_ids,
    hess_out,
    grad_out,
    cost_out,
    pts,
    pose_pad,
    send0,
    recv0,
    raw,
    table,
    world,
    vox_row,
    send1,
    recv1,
    moved,
    send2,
    recv2,
    back,
    terms,
    send3,
    recv3,
    pts_sem,
    sends,
    recvs,
):
    n_tm, n_map, slots, npoints, scale = sizes
    devices = n_tm * n_map
    blocks = pts.shape[1]
    chunks = blocks // LANES
    per = LANES // slots
    own_scans = poses.shape[1]
    spread = LANES // own_scans
    scans = own_scans * n_map
    wide = scans // LANES
    voxels = angles.shape[1]
    tm = lax.axis_index("tm")
    mp = lax.axis_index("map")
    me = tm * n_map + mp

    def place(q):
        return (q // n_map, lax.rem(q, n_map))

    def chunk_copy(r):
        rows = pl.ds(r * LANES, LANES)
        return pltpu.make_async_copy(points.at[:, rows, :], pts.at[:, rows, :], pts_sem.at[r])

    loop(chunks, lambda r: chunk_copy(r).start())
    barrier = pltpu.get_barrier_semaphore()

    def greet(i, carry):
        pl.semaphore_signal(
            barrier, inc=1, device_id=place(lax.rem(me + i, devices)), device_id_type=MESH
        )
        return carry

    lax.fori_loop(1, devices, greet, 0)

    lane = lax.broadcasted_iota(jnp.int32, (8, LANES), 1)

    pose_pad[...] = jnp.zeros_like(pose_pad)
    pose_pad[0:6, 0:own_scans] = poses[...]
    mine = lax.rem(mp, spread)
    pose = pltpu.roll(pose_pad[...], mine * own_scans, 1)
    here = (lane // own_scans)[0:1] == mine
    cos, sin = jnp.cos(pose), jnp.sin(pose)
    cx, cy, cz = cos[0:1], cos[1:2], cos[2:3]
    sx, sy, sz = sin[0:1], sin[1:2], sin[2:3]
    rows = [
        cz * cy,
        cz * sy * sx - sz * cx,
        cz * sy * cx + sz * sx,
        sz * cy,
        sz * sy * sx + cz * cx,
        sz * sy * cx - cz * sx,
        -sy,
        cy * sx,
        cy * cx,
        pose[3:4],
        pose[4:5],
        pose[5:6],
    ]
    send0[...] = jnp.zeros_like(send0)
    for k, row in enumerate(rows):
        send0[k : k + 1, :] = jnp.where(here, row, 0.0)
    recv0[mp] = send0[...]

    theta, phi = angles[0:1, :], angles[1:2, :]
    sin_theta = jnp.sin(theta)
    normal = [sin_theta * jnp.cos(phi), sin_theta * jnp.sin(phi), jnp.cos(theta)]

    def raw_moments(r):
        chunk_copy(r).wait()
        at = pl.ds(r * LANES, LANES)
        xyz = [pts[i, at, :].T for i in range(3)]
        sums = [jnp.sum(x, axis=0, keepdims=True) for x in xyz]
        sums += [jnp.sum(xyz[i] * xyz[j], axis=0, keepdims=True) for i, j in PAIRS]
        for k, row in enumerate(sums):
            raw[pl.ds(r * 16 + k, 1), :] = row

    half = chunks // 2
    loop(half, raw_moments)
    pl.semaphore_wait(barrier, devices - 1)

    def map_copy(i, source, dest, s):
        peer = lax.rem(mp + i, n_map)
        return pltpu.make_async_remote_copy(
            src_ref=source(peer),
            dst_ref=dest.at[mp],
            send_sem=sends.at[s],
            recv_sem=recvs.at[s],
            device_id=(tm, peer),
            device_id_type=MESH,
        )

    for i in range(1, n_map):
        map_copy(i, lambda peer: send0, recv0, 0).start()
    loop(chunks - half, lambda r: raw_moments(half + r))

    def wait_bytes(ref, sem):
        pltpu.make_async_copy(ref, ref, sem).wait()

    wait_bytes(recv0.at[pl.ds(0, n_map - 1)], recvs.at[0])

    halves = []
    for h in range(wide):
        total = recv0[h * spread]
        for a in range(1, spread):
            total = total + recv0[h * spread + a]
        halves.append(total)
    pose_parts = parts_of(jnp.concatenate(halves, axis=1))

    scan_iota = lax.broadcasted_iota(jnp.int32, (scans, LANES), 0)

    def scan_hot(r):
        return jnp.where(scan_ids[pl.ds(r, 1), :] == scan_iota, 1.0, 0.0).astype(jnp.bfloat16)

    def look_up(r):
        found = jnp.dot(pose_parts, scan_hot(r), preferred_element_type=jnp.float32)
        table[pl.ds(pl.multiple_of(r * 16, 16), 16), :] = joined(found)

    loop(chunks, look_up)

    def every(ref, k, stride):
        return ref[pl.ds(k, chunks, stride=stride), :]

    first = [every(raw, k, 16) for k in range(3)]
    second = [every(raw, 3 + k, 16) for k in range(6)]
    rot = [[every(table, 3 * i + j, 16) for j in range(3)] for i in range(3)]
    shift = [every(table, 9 + i, 16) for i in range(3)]
    turned = [sum(rot[i][j] * first[j] for j in range(3)) for i in range(3)]
    half_turned = [
        [sum(rot[i][k] * second[PAIR_ROW[(k, j)]] for k in range(3)) for j in range(3)]
        for i in range(3)
    ]
    m1 = [turned[i] + npoints * shift[i] for i in range(3)]
    m2 = [
        sum(half_turned[i][k] * rot[j][k] for k in range(3))
        + turned[i] * shift[j]
        + shift[i] * m1[j]
        for i, j in PAIRS
    ]
    ids = voxel_ids[...]
    row_of = lax.broadcasted_iota(jnp.int32, ids.shape, 0)
    lane_of = lax.broadcasted_iota(jnp.int32, ids.shape, 1)
    owner_of = row_of * per + lane_of // slots
    local_ids = jnp.where(ids >= 0, ids - owner_of * voxels, -1).astype(jnp.float32)
    world[...] = jnp.zeros_like(world)
    for k, value in enumerate(m1 + m2 + [local_ids]):
        world[pl.ds(8 * (k // 4) + k % 4, chunks, stride=24), :] = value

    group = lane // slots

    def pack(r):
        pieces = [world[pl.ds(pl.multiple_of(r * 24 + 8 * c, 8), 8), :] for c in range(3)]
        for g in range(per):
            send1[r * per + g] = group_turn(pieces, g, group, slots)[0:4]

    loop(chunks, pack)

    def all_copy(i, source, dest, s):
        peer = lax.rem(me + i, devices)
        return pltpu.make_async_remote_copy(
            src_ref=source(peer),
            dst_ref=dest.at[me],
            send_sem=sends.at[s],
            recv_sem=recvs.at[s],
            device_id=place(peer),
            device_id_type=MESH,
        )

    def send_all(source, dest, s):
        def step(i, carry):
            all_copy(i, source, dest, s).start()
            return carry

        lax.fori_loop(1, devices, step, 0)

    send_all(lambda peer: send1.at[peer], recv1, 1)
    recv1[me] = send1[me]
    wait_bytes(recv1.at[pl.ds(0, devices - 1)], recvs.at[1])

    vox_iota = lax.broadcasted_iota(jnp.int32, (voxels, LANES), 0).astype(jnp.float32)
    zero4 = jnp.zeros((4, LANES), jnp.float32)

    def unpack(r):
        pieces = [jnp.concatenate([recv1[r * per + g], zero4], axis=0) for g in range(per)]
        for c in range(3):
            moved[pl.ds(pl.multiple_of(r * 24 + 8 * c, 8), 8), :] = group_turn(
                pieces, c, group, slots
            )

    loop(chunks, unpack)

    def vox_hot(r):
        row = moved[pl.ds(r * 24 + 17, 1), :]
        return jnp.where(row == vox_iota, 1.0, 0.0).astype(jnp.bfloat16)

    contract_last = (((1,), (1,)), ((), ()))
    row_id = lax.broadcasted_iota(jnp.int32, (24, LANES), 0)

    def add_voxels(r, acc):
        values = moved[pl.ds(pl.multiple_of(r * 24, 8), 24), :]
        values = jnp.where(row_id == 17, 1.0, values)
        return acc + lax.dot_general(
            parts_of(values), vox_hot(r), contract_last, preferred_element_type=jnp.float32
        )

    def summed(body, rows, columns):
        acc = jnp.zeros((rows, columns), jnp.float32)
        if chunks <= 8:
            for r in range(chunks):
                acc = body(r, acc)
            return acc
        return lax.fori_loop(0, chunks, body, acc)

    sums = joined(summed(add_voxels, 72, voxels))
    s1 = [sums[0:1], sums[1:2], sums[2:3]]
    s2 = [sums[3:4], sums[8:9], sums[9:10], sums[10:11], sums[11:12], sums[16:17]]
    floor_count = jnp.maximum(sums[17:18] * npoints, 1.0)
    offset = sum(normal[i] * s1[i] for i in range(3)) / floor_count
    quadric = sum(normal[i] ** 2 * s2[i] for i in range(3)) + 2.0 * sum(
        normal[PAIRS[k][0]] * normal[PAIRS[k][1]] * s2[k] for k in range(3, 6)
    )
    cost_out[...] = quadric / floor_count - offset**2
    vox_row[...] = jnp.zeros_like(vox_row)
    for k, row in enumerate(normal + [offset]):
        vox_row[k : k + 1, :] = row
    reply_parts = parts_of(vox_row[...])

    def reply(r):
        found = jnp.dot(reply_parts, vox_hot(r), preferred_element_type=jnp.float32)
        send2[r] = joined(found)[0:4]

    loop(chunks, reply)
    send_all(lambda peer: send2.at[peer // per], recv2, 2)
    recv2[me] = send2[me // per]
    wait_bytes(recv2.at[pl.ds(0, devices - 1)], recvs.at[2])

    my_group = lax.rem(me, per)

    def unpack_reply(r):
        pieces = [jnp.concatenate([recv2[r * per + g], zero4], axis=0) for g in range(per)]
        back[pl.ds(pl.multiple_of(r * 8, 8), 8), :] = group_turn(pieces, my_group, group, slots)

    loop(chunks, unpack_reply)
    n = [every(back, c, 8) for c in range(3)]
    d = every(back, 3, 8)

    def skew(v):
        return [n[2] * v[1] - n[1] * v[2], n[0] * v[2] - n[2] * v[0], n[1] * v[0] - n[0] * v[1]]

    full = [[m2[PAIR_ROW[(i, j)]] for j in range(3)] for i in range(3)]
    columns = [skew([full[k][j] for k in range(3)]) for j in range(3)]
    left = [[columns[j][i] for j in range(3)] for i in range(3)]
    upper = [skew(left[i]) for i in range(3)]
    skew_first = skew(m1)
    found = {}
    for i in range(3):
        for j in range(3):
            if j >= i:
                found[("h", i, j)] = upper[i][j]
                found[("h", 3 + i, 3 + j)] = npoints * n[i] * n[j]
            found[("h", i, 3 + j)] = skew_first[i] * n[j]
    rest = n[0] * m1[0] + n[1] * m1[1] + n[2] * m1[2] - npoints * d
    for i in range(3):
        found[("g", i)] = sum(left[i][j] * n[j] for j in range(3)) - d * skew_first[i]
        found[("g", 3 + i)] = n[i] * rest
    row_for = {}
    for k, (name, value) in enumerate(found.items()):
        row_for[name] = k
        terms[pl.ds(k, chunks, stride=32), :] = value
    for k in range(len(found), 32):
        terms[pl.ds(k, chunks, stride=32), :] = jnp.zeros_like(d)

    def add_scans(r, acc):
        values = parts_of(terms[pl.ds(pl.multiple_of(r * 32, 32), 32), :])
        return acc + lax.dot_general(
            values, scan_hot(r), contract_last, preferred_element_type=jnp.float32
        )

    per_scan = joined(summed(add_scans, 96, scans)) * scale
    scan_group = lane // own_scans
    for h in range(wide):
        pieces = [
            per_scan[8 * c : 8 * c + 8, h * LANES : (h + 1) * LANES] for c in range(4)
        ]
        for b in range(spread):
            send3[h * spread + b] = group_turn(pieces, b, scan_group, own_scans)
    for i in range(1, n_map):
        map_copy(i, lambda peer: send3.at[peer], recv3, 3).start()
    recv3[mp] = send3[mp]
    wait_bytes(recv3.at[pl.ds(0, n_map - 1)], recvs.at[3])
    total = recv3[0]
    for m in range(1, n_map):
        total = total + recv3[m]
    lined = [total] + [pltpu.roll(total, LANES - own_scans * c, 1) for c in range(1, 4)]

    def row_at(k):
        return lined[k // 8][k % 8 : k % 8 + 1, 0:own_scans]

    for i in range(6):
        for j in range(6):
            hess_out[6 * i + j : 6 * i + j + 1, :] = row_at(
                row_for[("h", min(i, j), max(i, j))]
            )
        grad_out[i : i + 1, :] = row_at(row_for[("g", i)])

    wait_bytes(recv0.at[pl.ds(0, n_map - 1)], sends.at[0])
    wait_bytes(send1.at[pl.ds(0, devices - 1)], sends.at[1])
    wait_bytes(recv2.at[pl.ds(0, devices - 1)], sends.at[2])
    wait_bytes(send3.at[pl.ds(0, n_map - 1)], sends.at[3])


def local(points, poses, normal_angles, voxel_ids, scan_ids):
    blocks, npoints = points.shape[1:]
    n_tm, n_map = lax.axis_size("tm"), lax.axis_size("map")
    devices = n_tm * n_map
    slots = blocks // devices
    chunks = blocks // LANES
    vox_count = normal_angles.shape[1]
    own_scans = poses.shape[1]
    assert LANES % slots == 0 and own_scans * 4 == LANES and n_map % 4 == 0
    assert npoints == LANES and slots * 4 == LANES
    scale = own_scans * devices / (blocks * devices * npoints)
    f32 = jnp.float32
    vmem = pl.BlockSpec(memory_space=pltpu.VMEM)
    hess, grad, cost = pl.pallas_call(
        functools.partial(kernel, (n_tm, n_map, slots, float(npoints), scale)),
        out_shape=(
            jax.ShapeDtypeStruct((36, own_scans), f32),
            jax.ShapeDtypeStruct((6, own_scans), f32),
            jax.ShapeDtypeStruct((1, vox_count), f32),
        ),
        in_specs=[pl.BlockSpec(memory_space=pl.ANY)] + [vmem] * 4,
        out_specs=(vmem, vmem, vmem),
        scratch_shapes=[
            pltpu.VMEM(points.shape, f32),
            pltpu.VMEM((8, LANES), f32),
            pltpu.VMEM((16, LANES), f32),
            pltpu.VMEM((n_map, 16, LANES), f32),
            pltpu.VMEM((chunks * 16, LANES), f32),
            pltpu.VMEM((chunks * 16, LANES), f32),
            pltpu.VMEM((chunks * 24, LANES), f32),
            pltpu.VMEM((8, vox_count), f32),
            pltpu.VMEM((devices, 4, LANES), f32),
            pltpu.VMEM((devices, 4, LANES), f32),
            pltpu.VMEM((chunks * 24, LANES), f32),
            pltpu.VMEM((chunks, 4, LANES), f32),
            pltpu.VMEM((devices, 4, LANES), f32),
            pltpu.VMEM((chunks * 8, LANES), f32),
            pltpu.VMEM((chunks * 32, LANES), f32),
            pltpu.VMEM((n_map, 8, LANES), f32),
            pltpu.VMEM((n_map, 8, LANES), f32),
            pltpu.SemaphoreType.DMA((chunks,)),
            pltpu.SemaphoreType.DMA((4,)),
            pltpu.SemaphoreType.DMA((4,)),
        ],
        compiler_params=pltpu.CompilerParams(collective_id=0, has_side_effects=True),
    )(
        points,
        poses,
        normal_angles,
        voxel_ids.reshape(chunks, LANES),
        scan_ids.reshape(chunks, LANES),
    )
    return hess, grad, cost.reshape(vox_count)


def solution(mesh):
    return jax.shard_map(
        local,
        mesh=mesh,
        in_specs=(
            P(None, ("tm", "map"), None),
            P(None, ("tm", "map")),
            P(None, ("tm", "map")),
            P(("tm", "map")),
            P(("tm", "map")),
        ),
        out_specs=(P(None, ("tm", "map")), P(None, ("tm", "map")), P(("tm", "map"))),
        check_vma=False,
    )
```

```python
import functools

import jax
import jax.numpy as jnp
from jax import lax
from jax.experimental import pallas as pl
from jax.experimental.pallas import tpu as pltpu
from jax.sharding import PartitionSpec as P

LANES = 128
MESH = pl.DeviceIdType.MESH
PAIRS = [(0, 0), (1, 1), (2, 2), (0, 1), (0, 2), (1, 2)]
PAIR_ROW = {}
for _k, (_i, _j) in enumerate(PAIRS):
    PAIR_ROW[(_i, _j)] = _k
    PAIR_ROW[(_j, _i)] = _k


ROWS = [("h", i, j) for i in range(6) for j in range(i, 6)] + [("g", i) for i in range(6)]


def parts_of(x):
    high = x.astype(jnp.bfloat16)
    rest = x - high.astype(jnp.float32)
    mid = rest.astype(jnp.bfloat16)
    low = (rest - mid.astype(jnp.float32)).astype(jnp.bfloat16)
    return jnp.concatenate([high, mid, low], axis=0)


def joined(y):
    rows = y.shape[0] // 3
    return y[:rows] + y[rows : 2 * rows] + y[2 * rows :]


def group_turn(pieces, out_group, group, lanes_per):
    total = None
    for a, piece in enumerate(pieces):
        shift = lax.rem((a - out_group) * lanes_per + LANES, LANES)
        if isinstance(out_group, int):
            shift = ((a - out_group) * lanes_per) % LANES
        moved = piece if isinstance(shift, int) and shift == 0 else pltpu.roll(piece, shift, 1)
        total = moved if total is None else jnp.where(group == a, moved, total)
    return total


def loop(count, body):
    if count <= 8:
        for i in range(count):
            body(i)
    else:
        def step(i, carry):
            body(i)
            return carry

        lax.fori_loop(0, count, step, 0)


def kernel(
    sizes,
    points,
    poses,
    angles,
    voxel_ids,
    scan_ids,
    packed,
    pts,
    pose_pad,
    send0,
    recv0,
    raw,
    table,
    world,
    vox_row,
    send1,
    recv1,
    moved,
    send2,
    recv2,
    back,
    terms,
    send3,
    recv3,
    pts_sem,
    sends,
    recvs,
):
    n_tm, n_map, slots, npoints, scale = sizes
    devices = n_tm * n_map
    blocks = pts.shape[1]
    chunks = blocks // LANES
    per = LANES // slots
    own_scans = poses.shape[1]
    spread = LANES // own_scans
    scans = own_scans * n_map
    wide = scans // LANES
    voxels = angles.shape[1]
    tm = lax.axis_index("tm")
    mp = lax.axis_index("map")
    me = tm * n_map + mp

    def place(q):
        return (q // n_map, lax.rem(q, n_map))

    def chunk_copy(r):
        rows = pl.ds(r * LANES, LANES)
        return pltpu.make_async_copy(points.at[:, rows, :], pts.at[:, rows, :], pts_sem.at[r])

    loop(chunks, lambda r: chunk_copy(r).start())
    barrier = pltpu.get_barrier_semaphore()

    def greet(i, carry):
        pl.semaphore_signal(
            barrier, inc=1, device_id=place(lax.rem(me + i, devices)), device_id_type=MESH
        )
        return carry

    lax.fori_loop(1, devices, greet, 0)

    lane = lax.broadcasted_iota(jnp.int32, (8, LANES), 1)

    pose_pad[...] = jnp.zeros_like(pose_pad)
    pose_pad[0:6, 0:own_scans] = poses[...]
    mine = lax.rem(mp, spread)
    pose = pltpu.roll(pose_pad[...], mine * own_scans, 1)
    here = (lane // own_scans)[0:1] == mine
    cos, sin = jnp.cos(pose), jnp.sin(pose)
    cx, cy, cz = cos[0:1], cos[1:2], cos[2:3]
    sx, sy, sz = sin[0:1], sin[1:2], sin[2:3]
    rows = [
        cz * cy,
        cz * sy * sx - sz * cx,
        cz * sy * cx + sz * sx,
        sz * cy,
        sz * sy * sx + cz * cx,
        sz * sy * cx - cz * sx,
        -sy,
        cy * sx,
        cy * cx,
        pose[3:4],
        pose[4:5],
        pose[5:6],
    ]
    send0[...] = jnp.zeros_like(send0)
    for k, row in enumerate(rows):
        send0[k : k + 1, :] = jnp.where(here, row, 0.0)
    recv0[mp] = send0[...]

    theta, phi = angles[0:1, :], angles[1:2, :]
    sin_theta = jnp.sin(theta)
    normal = [sin_theta * jnp.cos(phi), sin_theta * jnp.sin(phi), jnp.cos(theta)]

    def raw_moments(r):
        chunk_copy(r).wait()
        at = pl.ds(r * LANES, LANES)
        xyz = [pts[i, at, :].T for i in range(3)]
        sums = [jnp.sum(x, axis=0, keepdims=True) for x in xyz]
        sums += [jnp.sum(xyz[i] * xyz[j], axis=0, keepdims=True) for i, j in PAIRS]
        for k, row in enumerate(sums):
            raw[pl.ds(r * 16 + k, 1), :] = row

    half = chunks // 2
    loop(half, raw_moments)
    pl.semaphore_wait(barrier, devices - 1)

    def map_copy(i, source, dest, s):
        peer = lax.rem(mp + i, n_map)
        return pltpu.make_async_remote_copy(
            src_ref=source(peer),
            dst_ref=dest.at[mp],
            send_sem=sends.at[s],
            recv_sem=recvs.at[s],
            device_id=(tm, peer),
            device_id_type=MESH,
        )

    for i in range(1, n_map):
        map_copy(i, lambda peer: send0, recv0, 0).start()
    loop(chunks - half, lambda r: raw_moments(half + r))

    def wait_bytes(ref, sem):
        pltpu.make_async_copy(ref, ref, sem).wait()

    wait_bytes(recv0.at[pl.ds(0, n_map - 1)], recvs.at[0])

    halves = []
    for h in range(wide):
        total = recv0[h * spread]
        for a in range(1, spread):
            total = total + recv0[h * spread + a]
        halves.append(total)
    pose_parts = parts_of(jnp.concatenate(halves, axis=1))

    scan_iota = lax.broadcasted_iota(jnp.int32, (scans, LANES), 0)

    def scan_hot(r):
        return jnp.where(scan_ids[pl.ds(r, 1), :] == scan_iota, 1.0, 0.0).astype(jnp.bfloat16)

    def look_up(r):
        found = jnp.dot(pose_parts, scan_hot(r), preferred_element_type=jnp.float32)
        table[pl.ds(pl.multiple_of(r * 16, 16), 16), :] = joined(found)

    loop(chunks, look_up)

    def every(ref, k, stride):
        return ref[pl.ds(k, chunks, stride=stride), :]

    first = [every(raw, k, 16) for k in range(3)]
    second = [every(raw, 3 + k, 16) for k in range(6)]
    rot = [[every(table, 3 * i + j, 16) for j in range(3)] for i in range(3)]
    shift = [every(table, 9 + i, 16) for i in range(3)]
    turned = [sum(rot[i][j] * first[j] for j in range(3)) for i in range(3)]
    half_turned = [
        [sum(rot[i][k] * second[PAIR_ROW[(k, j)]] for k in range(3)) for j in range(3)]
        for i in range(3)
    ]
    m1 = [turned[i] + npoints * shift[i] for i in range(3)]
    m2 = [
        sum(half_turned[i][k] * rot[j][k] for k in range(3))
        + turned[i] * shift[j]
        + shift[i] * m1[j]
        for i, j in PAIRS
    ]
    ids = voxel_ids[...]
    row_of = lax.broadcasted_iota(jnp.int32, ids.shape, 0)
    lane_of = lax.broadcasted_iota(jnp.int32, ids.shape, 1)
    owner_of = row_of * per + lane_of // slots
    local_ids = jnp.where(ids >= 0, ids - owner_of * voxels, -1).astype(jnp.float32)
    world[...] = jnp.zeros_like(world)
    for k, value in enumerate(m1 + m2 + [local_ids]):
        world[pl.ds(8 * (k // 4) + k % 4, chunks, stride=24), :] = value

    group = lane // slots

    def pack(r):
        pieces = [world[pl.ds(pl.multiple_of(r * 24 + 8 * c, 8), 8), :] for c in range(3)]
        for g in range(per):
            send1[r * per + g] = group_turn(pieces, g, group, slots)[0:4]

    loop(chunks, pack)

    upper = tm // (n_tm // 2)

    def all_copy(i, source, dest, s):
        step = lax.rem(i, devices) // n_map
        tm_peer = (1 - upper) * (n_tm - 1 - step) + upper * step
        peer = tm_peer * n_map + lax.rem(mp + i, n_map)
        return pltpu.make_async_remote_copy(
            src_ref=source(peer),
            dst_ref=dest.at[me],
            send_sem=sends.at[s],
            recv_sem=recvs.at[s],
            device_id=place(peer),
            device_id_type=MESH,
        ), peer

    def send_all(source, dest, s):
        def start_with(i, carry):
            copy, peer = all_copy(i, source, dest, s)

            @pl.when(peer != me)
            def _():
                copy.start()

            return carry

        lax.fori_loop(0, devices, start_with, 0, unroll=4)

    send_all(lambda peer: send1.at[peer], recv1, 1)
    recv1[me] = send1[me]
    wait_bytes(recv1.at[pl.ds(0, devices - 1)], recvs.at[1])

    vox_iota = lax.broadcasted_iota(jnp.int32, (voxels, LANES), 0).astype(jnp.float32)
    zero4 = jnp.zeros((4, LANES), jnp.float32)

    def unpack(r):
        pieces = [jnp.concatenate([recv1[r * per + g], zero4], axis=0) for g in range(per)]
        for c in range(3):
            moved[pl.ds(pl.multiple_of(r * 24 + 8 * c, 8), 8), :] = group_turn(
                pieces, c, group, slots
            )

    loop(chunks, unpack)

    def vox_hot(r):
        row = moved[pl.ds(r * 24 + 17, 1), :]
        return jnp.where(row == vox_iota, 1.0, 0.0).astype(jnp.bfloat16)

    contract_last = (((1,), (1,)), ((), ()))
    row_id = lax.broadcasted_iota(jnp.int32, (24, LANES), 0)

    def add_voxels(r, acc):
        values = moved[pl.ds(pl.multiple_of(r * 24, 8), 24), :]
        values = jnp.where(row_id == 17, 1.0, values)
        return acc + lax.dot_general(
            parts_of(values), vox_hot(r), contract_last, preferred_element_type=jnp.float32
        )

    def summed(body, rows, columns):
        acc = jnp.zeros((rows, columns), jnp.float32)
        if chunks <= 8:
            for r in range(chunks):
                acc = body(r, acc)
            return acc
        return lax.fori_loop(0, chunks, body, acc)

    sums = joined(summed(add_voxels, 72, voxels))
    s1 = [sums[0:1], sums[1:2], sums[2:3]]
    s2 = [sums[3:4], sums[8:9], sums[9:10], sums[10:11], sums[11:12], sums[16:17]]
    floor_count = jnp.maximum(sums[17:18] * npoints, 1.0)
    offset = sum(normal[i] * s1[i] for i in range(3)) / floor_count
    quadric = sum(normal[i] ** 2 * s2[i] for i in range(3)) + 2.0 * sum(
        normal[PAIRS[k][0]] * normal[PAIRS[k][1]] * s2[k] for k in range(3, 6)
    )
    cost = quadric / floor_count - offset**2
    for h in range(voxels // LANES):
        packed[8 + h : 9 + h, :] = cost[:, h * LANES : (h + 1) * LANES]
    vox_row[...] = jnp.zeros_like(vox_row)
    for k, row in enumerate(normal + [offset]):
        vox_row[k : k + 1, :] = row
    reply_parts = parts_of(vox_row[...])

    def reply(r):
        found = jnp.dot(reply_parts, vox_hot(r), preferred_element_type=jnp.float32)
        value = joined(found)
        rolled = [value] + [pltpu.roll(value, slots * a, 1) for a in range(1, per)]
        for g in range(per):
            total = jnp.zeros_like(value)
            for c in range(4):
                total = jnp.where(corner & (group == c), rolled[(c - g) % per], total)
            send2[r * per + g] = jnp.sum(total, axis=0, keepdims=True)

    corner = lax.broadcasted_iota(jnp.int32, (8, LANES), 0) == group
    loop(chunks, reply)
    send_all(lambda peer: send2.at[peer], recv2, 2)
    recv2[me] = send2[me]
    wait_bytes(recv2.at[pl.ds(0, devices - 1)], recvs.at[2])

    back[...] = recv2[...].reshape(devices, LANES)
    pieces = [back[pl.ds(g, chunks, stride=per), :] for g in range(per)]
    wide_group = lane_of // slots
    n = [group_turn(pieces, c, wide_group, slots) for c in range(3)]
    d = group_turn(pieces, 3, wide_group, slots)

    def skew(v):
        return [n[2] * v[1] - n[1] * v[2], n[0] * v[2] - n[2] * v[0], n[1] * v[0] - n[0] * v[1]]

    full = [[m2[PAIR_ROW[(i, j)]] for j in range(3)] for i in range(3)]
    columns = [skew([full[k][j] for k in range(3)]) for j in range(3)]
    left = [[columns[j][i] for j in range(3)] for i in range(3)]
    corner_block = [skew(left[i]) for i in range(3)]
    skew_first = skew(m1)
    found = {}
    for i in range(3):
        for j in range(3):
            if j >= i:
                found[("h", i, j)] = corner_block[i][j]
                found[("h", 3 + i, 3 + j)] = npoints * n[i] * n[j]
            found[("h", i, 3 + j)] = skew_first[i] * n[j]
    rest = n[0] * m1[0] + n[1] * m1[1] + n[2] * m1[2] - npoints * d
    for i in range(3):
        found[("g", i)] = sum(left[i][j] * n[j] for j in range(3)) - d * skew_first[i]
        found[("g", 3 + i)] = n[i] * rest
    for name, value in found.items():
        k = ROWS.index(name)
        terms[pl.ds(k, chunks, stride=32), :] = value
    for k in range(len(found), 32):
        terms[pl.ds(k, chunks, stride=32), :] = jnp.zeros_like(d)

    def add_scans(r, acc):
        values = parts_of(terms[pl.ds(pl.multiple_of(r * 32, 32), 32), :])
        return acc + lax.dot_general(
            values, scan_hot(r), contract_last, preferred_element_type=jnp.float32
        )

    per_scan = joined(summed(add_scans, 96, scans)) * scale
    scan_group = lane // own_scans
    for h in range(wide):
        pieces = [
            per_scan[8 * c : 8 * c + 8, h * LANES : (h + 1) * LANES] for c in range(4)
        ]
        for b in range(spread):
            send3[h * spread + b] = group_turn(pieces, b, scan_group, own_scans)
    for i in range(1, n_map):
        map_copy(i, lambda peer: send3.at[peer], recv3, 3).start()
    recv3[mp] = send3[mp]
    wait_bytes(recv3.at[pl.ds(0, n_map - 1)], recvs.at[3])
    total = recv3[0]
    for m in range(1, n_map):
        total = total + recv3[m]
    packed[0:8, :] = total

    wait_bytes(recv0.at[pl.ds(0, n_map - 1)], sends.at[0])
    wait_bytes(send1.at[pl.ds(0, devices - 1)], sends.at[1])
    wait_bytes(recv2.at[pl.ds(0, devices - 1)], sends.at[2])
    wait_bytes(send3.at[pl.ds(0, n_map - 1)], sends.at[3])


def finish(packed, hess_out, grad_out, cost_out, lines):
    own_scans = grad_out.shape[1]
    total = packed[0:8, :]
    lined = [total] + [pltpu.roll(total, LANES - own_scans * c, 1) for c in range(1, 4)]

    def row_at(name):
        k = ROWS.index(name)
        return lined[k // 8][k % 8 : k % 8 + 1]

    lines[...] = jnp.zeros_like(lines)
    for i in range(6):
        for j in range(6):
            lines[6 * i + j : 6 * i + j + 1, :] = row_at(("h", min(i, j), max(i, j)))
        grad_out[i : i + 1, :] = row_at(("g", i))[:, 0:own_scans]
    hess_out[...] = lines[...].T[0:own_scans, 0:36]
    for h in range(cost_out.shape[1] // LANES):
        cost_out[:, h * LANES : (h + 1) * LANES] = packed[8 + h : 9 + h, :]


def local(points, poses, normal_angles, voxel_ids, scan_ids):
    blocks, npoints = points.shape[1:]
    n_tm, n_map = lax.axis_size("tm"), lax.axis_size("map")
    devices = n_tm * n_map
    slots = blocks // devices
    chunks = blocks // LANES
    vox_count = normal_angles.shape[1]
    own_scans = poses.shape[1]
    assert LANES % slots == 0 and own_scans * 4 == LANES and n_map % 4 == 0
    assert npoints == LANES and slots * 4 == LANES
    scale = own_scans * devices / (blocks * devices * npoints)
    f32 = jnp.float32
    vmem = pl.BlockSpec(memory_space=pltpu.VMEM)
    extra = -(-(vox_count // LANES) // 8) * 8
    packed = pl.pallas_call(
        functools.partial(kernel, (n_tm, n_map, slots, float(npoints), scale)),
        out_shape=jax.ShapeDtypeStruct((8 + extra, LANES), f32),
        in_specs=[pl.BlockSpec(memory_space=pl.ANY)] + [vmem] * 4,
        out_specs=vmem,
        scratch_shapes=[
            pltpu.VMEM(points.shape, f32),
            pltpu.VMEM((8, LANES), f32),
            pltpu.VMEM((16, LANES), f32),
            pltpu.VMEM((n_map, 16, LANES), f32),
            pltpu.VMEM((chunks * 16, LANES), f32),
            pltpu.VMEM((chunks * 16, LANES), f32),
            pltpu.VMEM((chunks * 24, LANES), f32),
            pltpu.VMEM((8, vox_count), f32),
            pltpu.VMEM((devices, 4, LANES), f32),
            pltpu.VMEM((devices, 4, LANES), f32),
            pltpu.VMEM((chunks * 24, LANES), f32),
            pltpu.VMEM((devices, 1, LANES), f32),
            pltpu.VMEM((devices, 1, LANES), f32),
            pltpu.VMEM((devices, LANES), f32),
            pltpu.VMEM((chunks * 32, LANES), f32),
            pltpu.VMEM((n_map, 8, LANES), f32),
            pltpu.VMEM((n_map, 8, LANES), f32),
            pltpu.SemaphoreType.DMA((chunks,)),
            pltpu.SemaphoreType.DMA((4,)),
            pltpu.SemaphoreType.DMA((4,)),
        ],
        compiler_params=pltpu.CompilerParams(collective_id=0, has_side_effects=True),
    )(
        points,
        poses,
        normal_angles,
        voxel_ids.reshape(chunks, LANES),
        scan_ids.reshape(chunks, LANES),
    )
    hess, grad, cost = pl.pallas_call(
        finish,
        out_shape=(
            jax.ShapeDtypeStruct((own_scans, 36), f32),
            jax.ShapeDtypeStruct((6, own_scans), f32),
            jax.ShapeDtypeStruct((1, vox_count), f32),
        ),
        in_specs=[vmem],
        out_specs=(vmem, vmem, vmem),
        scratch_shapes=[pltpu.VMEM((LANES, LANES), f32)],
    )(packed)
    return hess.T, grad, cost.reshape(vox_count)


def solution(mesh):
    return jax.shard_map(
        local,
        mesh=mesh,
        in_specs=(
            P(None, ("tm", "map"), None),
            P(None, ("tm", "map")),
            P(None, ("tm", "map")),
            P(("tm", "map")),
            P(("tm", "map")),
        ),
        out_specs=(P(None, ("tm", "map")), P(None, ("tm", "map")), P(("tm", "map"))),
        check_vma=False,
    )
```

```python
import functools

import jax
import jax.numpy as jnp
from jax import lax
from jax.experimental import pallas as pl
from jax.experimental.pallas import tpu as pltpu
from jax.sharding import PartitionSpec as P

LANES = 128
MESH = pl.DeviceIdType.MESH
PAIRS = [(0, 0), (1, 1), (2, 2), (0, 1), (0, 2), (1, 2)]
PAIR_ROW = {}
for _k, (_i, _j) in enumerate(PAIRS):
    PAIR_ROW[(_i, _j)] = _k
    PAIR_ROW[(_j, _i)] = _k


ROWS = [("h", i, j) for i in range(6) for j in range(i, 6)] + [("g", i) for i in range(6)]


def parts_of(x):
    high = x.astype(jnp.bfloat16)
    rest = x - high.astype(jnp.float32)
    mid = rest.astype(jnp.bfloat16)
    low = (rest - mid.astype(jnp.float32)).astype(jnp.bfloat16)
    return jnp.concatenate([high, mid, low], axis=0)


def joined(y):
    rows = y.shape[0] // 3
    return y[:rows] + y[rows : 2 * rows] + y[2 * rows :]


def group_turn(pieces, out_group, group, lanes_per):
    total = None
    for a, piece in enumerate(pieces):
        shift = lax.rem((a - out_group) * lanes_per + LANES, LANES)
        if isinstance(out_group, int):
            shift = ((a - out_group) * lanes_per) % LANES
        moved = piece if isinstance(shift, int) and shift == 0 else pltpu.roll(piece, shift, 1)
        total = moved if total is None else jnp.where(group == a, moved, total)
    return total


def loop(count, body):
    if count <= 8:
        for i in range(count):
            body(i)
    else:
        def step(i, carry):
            body(i)
            return carry

        lax.fori_loop(0, count, step, 0)


def kernel(
    sizes,
    points,
    poses,
    angles,
    voxel_ids,
    scan_ids,
    packed,
    pts,
    pose_pad,
    table,
    sent,
    world,
    vox_row,
    send1,
    recv1,
    moved,
    send2,
    recv2,
    back,
    terms,
    send3,
    recv3,
    pts_sem,
    sends,
    recvs,
):
    n_tm, n_map, slots, npoints, scale = sizes
    devices = n_tm * n_map
    blocks = pts.shape[1]
    chunks = blocks // LANES
    per = LANES // slots
    own_scans = poses.shape[1]
    spread = LANES // own_scans
    scans = own_scans * n_map
    wide = scans // LANES
    voxels = angles.shape[1]
    tm = lax.axis_index("tm")
    mp = lax.axis_index("map")
    me = tm * n_map + mp

    def place(q):
        return (q // n_map, lax.rem(q, n_map))

    def chunk_copy(r):
        rows = pl.ds(r * LANES, LANES)
        return pltpu.make_async_copy(points.at[:, rows, :], pts.at[:, rows, :], pts_sem.at[r])

    loop(chunks, lambda r: chunk_copy(r).start())
    barrier = pltpu.get_barrier_semaphore()

    def greet(i, carry):
        pl.semaphore_signal(
            barrier, inc=1, device_id=place(lax.rem(me + i, devices)), device_id_type=MESH
        )
        return carry

    lax.fori_loop(1, devices, greet, 0)

    lane = lax.broadcasted_iota(jnp.int32, (8, LANES), 1)

    pose_pad[...] = jnp.zeros_like(pose_pad)
    for g in range(spread):
        pose_pad[0:6, g * own_scans : (g + 1) * own_scans] = poses[...]
    pose = pose_pad[...]
    cos, sin = jnp.cos(pose), jnp.sin(pose)
    cx, cy, cz = cos[0:1], cos[1:2], cos[2:3]
    sx, sy, sz = sin[0:1], sin[1:2], sin[2:3]
    rows = [
        cz * cy,
        cz * sy * sx - sz * cx,
        cz * sy * cx + sz * sx,
        sz * cy,
        sz * sy * sx + cz * cx,
        sz * sy * cx - cz * sx,
        -sy,
        cy * sx,
        cy * cx,
        pose[3:4],
        pose[4:5],
        pose[5:6],
    ]
    sent[...] = jnp.zeros_like(sent)

    def sent_row(k):
        return 8 * (k // 6) + k % 6

    for k, row in enumerate(rows):
        sent[pl.ds(sent_row(11 + k), chunks, stride=32), :] = jnp.broadcast_to(
            row, (chunks, LANES)
        )
    ids = voxel_ids[...]
    row_of = lax.broadcasted_iota(jnp.int32, ids.shape, 0)
    lane_of = lax.broadcasted_iota(jnp.int32, ids.shape, 1)
    owner_of = row_of * per + lane_of // slots
    local_ids = jnp.where(ids >= 0, ids - owner_of * voxels, -1).astype(jnp.float32)
    sent[pl.ds(sent_row(9), chunks, stride=32), :] = local_ids
    sent[pl.ds(sent_row(10), chunks, stride=32), :] = scan_ids[...].astype(jnp.float32)

    theta, phi = angles[0:1, :], angles[1:2, :]
    sin_theta = jnp.sin(theta)
    normal = [sin_theta * jnp.cos(phi), sin_theta * jnp.sin(phi), jnp.cos(theta)]

    def raw_moments(r):
        chunk_copy(r).wait()
        at = pl.ds(r * LANES, LANES)
        xyz = [pts[i, at, :].T for i in range(3)]
        sums = [jnp.sum(x, axis=0, keepdims=True) for x in xyz]
        sums += [jnp.sum(xyz[i] * xyz[j], axis=0, keepdims=True) for i, j in PAIRS]
        for k, row in enumerate(sums):
            sent[pl.ds(r * 32 + sent_row(k), 1), :] = row

    group = lane // slots

    def pack(r):
        raw_moments(r)
        pieces = [sent[pl.ds(pl.multiple_of(r * 32 + 8 * c, 8), 8), :] for c in range(4)]
        for g in range(per):
            send1[r * per + g] = group_turn(pieces, g, group, slots)[0:6]

    loop(chunks, pack)
    pl.semaphore_wait(barrier, devices - 1)

    def map_copy(i, source, dest, s):
        peer = lax.rem(mp + i, n_map)
        return pltpu.make_async_remote_copy(
            src_ref=source(peer),
            dst_ref=dest.at[mp],
            send_sem=sends.at[s],
            recv_sem=recvs.at[s],
            device_id=(tm, peer),
            device_id_type=MESH,
        )

    def wait_bytes(ref, sem):
        pltpu.make_async_copy(ref, ref, sem).wait()

    scan_iota = lax.broadcasted_iota(jnp.int32, (scans, LANES), 0)

    def scan_hot(r):
        return jnp.where(scan_ids[pl.ds(r, 1), :] == scan_iota, 1.0, 0.0).astype(jnp.bfloat16)

    def every(ref, k, stride):
        return ref[pl.ds(k, chunks, stride=stride), :]

    def transformed(source):
        first = [every(source, sent_row(k), 32) for k in range(3)]
        second = [every(source, sent_row(3 + k), 32) for k in range(6)]
        pose_at = [every(table, sent_row(11 + k) - 8, 24) for k in range(12)]
        rot = [pose_at[3 * i : 3 * i + 3] for i in range(3)]
        shift = pose_at[9:]
        turned = [sum(rot[i][j] * first[j] for j in range(3)) for i in range(3)]
        half_turned = [
            [sum(rot[i][k] * second[PAIR_ROW[(k, j)]] for k in range(3)) for j in range(3)]
            for i in range(3)
        ]
        m1 = [turned[i] + npoints * shift[i] for i in range(3)]
        m2 = [
            sum(half_turned[i][k] * rot[j][k] for k in range(3))
            + turned[i] * shift[j]
            + shift[i] * m1[j]
            for i, j in PAIRS
        ]
        return m1, m2

    upper = tm // (n_tm // 2)

    def all_copy(i, source, dest, s):
        step = lax.rem(i, devices) // n_map
        tm_peer = (1 - upper) * (n_tm - 1 - step) + upper * step
        peer = tm_peer * n_map + lax.rem(mp + i, n_map)
        return pltpu.make_async_remote_copy(
            src_ref=source(peer),
            dst_ref=dest.at[me],
            send_sem=sends.at[s],
            recv_sem=recvs.at[s],
            device_id=place(peer),
            device_id_type=MESH,
        ), peer

    def send_all(source, dest, s):
        def start_with(i, carry):
            copy, peer = all_copy(i, source, dest, s)

            @pl.when(peer != me)
            def _():
                copy.start()

            return carry

        lax.fori_loop(0, devices, start_with, 0, unroll=4)

    send_all(lambda peer: send1.at[peer], recv1, 1)
    recv1[me] = send1[me]
    wait_bytes(recv1.at[pl.ds(0, devices - 1)], recvs.at[1])

    vox_iota = lax.broadcasted_iota(jnp.int32, (voxels, LANES), 0).astype(jnp.float32)
    zero2 = jnp.zeros((2, LANES), jnp.float32)

    def unpack(r):
        pieces = [jnp.concatenate([recv1[r * per + g], zero2], axis=0) for g in range(per)]
        for c in range(4):
            moved[pl.ds(pl.multiple_of(r * 32 + 8 * c, 8), 8), :] = group_turn(
                pieces, c, group, slots
            )

    loop(chunks, unpack)

    def vox_hot(r):
        row = moved[pl.ds(r * 32 + sent_row(9), 1), :]
        return jnp.where(row == vox_iota, 1.0, 0.0).astype(jnp.bfloat16)

    float_iota = scan_iota.astype(jnp.float32)

    def group_parts(t):
        return parts_of(
            jnp.concatenate(
                [
                    moved[pl.ds(pl.multiple_of((t * wide + h) * 32 + 8, 8), 24), :]
                    for h in range(wide)
                ],
                axis=1,
            )
        )

    def look_up(t):
        table_parts = group_parts(t)
        for h in range(wide):
            r = t * wide + h
            row = moved[pl.ds(r * 32 + sent_row(10), 1), :]
            hot = jnp.where(row == float_iota, 1.0, 0.0).astype(jnp.bfloat16)
            found = jnp.dot(table_parts, hot, preferred_element_type=jnp.float32)
            table[pl.ds(pl.multiple_of(r * 24, 8), 24), :] = joined(found)

    loop(n_tm, look_up)
    m1, m2 = transformed(moved)
    world[...] = jnp.ones_like(world)
    for k, value in enumerate(m1 + m2):
        world[pl.ds(k, chunks, stride=16), :] = value

    contract_last = (((1,), (1,)), ((), ()))
    def add_voxels(r, acc):
        values = world[pl.ds(pl.multiple_of(r * 16, 16), 16), :]
        return acc + lax.dot_general(
            parts_of(values), vox_hot(r), contract_last, preferred_element_type=jnp.float32
        )

    def summed(body, rows, columns):
        acc = jnp.zeros((rows, columns), jnp.float32)
        if chunks <= 8:
            for r in range(chunks):
                acc = body(r, acc)
            return acc
        return lax.fori_loop(0, chunks, body, acc)

    sums = joined(summed(add_voxels, 48, voxels))
    s1 = [sums[k : k + 1] for k in range(3)]
    s2 = [sums[3 + k : 4 + k] for k in range(6)]
    floor_count = jnp.maximum(sums[9:10] * npoints, 1.0)
    offset = sum(normal[i] * s1[i] for i in range(3)) / floor_count
    quadric = sum(normal[i] ** 2 * s2[i] for i in range(3)) + 2.0 * sum(
        normal[PAIRS[k][0]] * normal[PAIRS[k][1]] * s2[k] for k in range(3, 6)
    )
    cost = quadric / floor_count - offset**2
    for h in range(voxels // LANES):
        packed[8 + h : 9 + h, :] = cost[:, h * LANES : (h + 1) * LANES]
    vox_row[...] = jnp.zeros_like(vox_row)
    for k, row in enumerate(normal + [offset]):
        vox_row[k : k + 1, :] = row
    reply_parts = parts_of(vox_row[...])

    def reply(r):
        found = jnp.dot(reply_parts, vox_hot(r), preferred_element_type=jnp.float32)
        value = joined(found)
        rolled = [value] + [pltpu.roll(value, slots * a, 1) for a in range(1, per)]
        for g in range(per):
            total = jnp.zeros_like(value)
            for c in range(4):
                total = jnp.where(corner & (group == c), rolled[(c - g) % per], total)
            send2[r * per + g] = jnp.sum(total, axis=0, keepdims=True)

    corner = lax.broadcasted_iota(jnp.int32, (8, LANES), 0) == group
    loop(chunks, reply)
    send_all(lambda peer: send2.at[peer], recv2, 2)
    recv2[me] = send2[me]

    own_parts = group_parts(tm)

    def look_up_own(r):
        found = jnp.dot(own_parts, scan_hot(r), preferred_element_type=jnp.float32)
        table[pl.ds(pl.multiple_of(r * 24, 8), 24), :] = joined(found)

    loop(chunks, look_up_own)
    m1, m2 = transformed(sent)
    wait_bytes(recv2.at[pl.ds(0, devices - 1)], recvs.at[2])

    back[...] = recv2[...].reshape(devices, LANES)
    pieces = [back[pl.ds(g, chunks, stride=per), :] for g in range(per)]
    wide_group = lane_of // slots
    n = [group_turn(pieces, c, wide_group, slots) for c in range(3)]
    d = group_turn(pieces, 3, wide_group, slots)

    def skew(v):
        return [n[2] * v[1] - n[1] * v[2], n[0] * v[2] - n[2] * v[0], n[1] * v[0] - n[0] * v[1]]

    full = [[m2[PAIR_ROW[(i, j)]] for j in range(3)] for i in range(3)]
    columns = [skew([full[k][j] for k in range(3)]) for j in range(3)]
    left = [[columns[j][i] for j in range(3)] for i in range(3)]
    corner_block = [skew(left[i]) for i in range(3)]
    skew_first = skew(m1)
    found = {}
    for i in range(3):
        for j in range(3):
            if j >= i:
                found[("h", i, j)] = corner_block[i][j]
                found[("h", 3 + i, 3 + j)] = npoints * n[i] * n[j]
            found[("h", i, 3 + j)] = skew_first[i] * n[j]
    rest = n[0] * m1[0] + n[1] * m1[1] + n[2] * m1[2] - npoints * d
    for i in range(3):
        found[("g", i)] = sum(left[i][j] * n[j] for j in range(3)) - d * skew_first[i]
        found[("g", 3 + i)] = n[i] * rest
    for name, value in found.items():
        k = ROWS.index(name)
        terms[pl.ds(k, chunks, stride=32), :] = value
    for k in range(len(found), 32):
        terms[pl.ds(k, chunks, stride=32), :] = jnp.zeros_like(d)

    def add_scans(r, acc):
        values = parts_of(terms[pl.ds(pl.multiple_of(r * 32, 32), 32), :])
        return acc + lax.dot_general(
            values, scan_hot(r), contract_last, preferred_element_type=jnp.float32
        )

    per_scan = joined(summed(add_scans, 96, scans)) * scale
    scan_group = lane // own_scans
    for h in range(wide):
        pieces = [
            per_scan[8 * c : 8 * c + 8, h * LANES : (h + 1) * LANES] for c in range(4)
        ]
        for b in range(spread):
            send3[h * spread + b] = group_turn(pieces, b, scan_group, own_scans)
    for i in range(1, n_map):
        map_copy(i, lambda peer: send3.at[peer], recv3, 0).start()
    recv3[mp] = send3[mp]
    wait_bytes(recv3.at[pl.ds(0, n_map - 1)], recvs.at[0])
    total = recv3[0]
    for m in range(1, n_map):
        total = total + recv3[m]
    packed[0:8, :] = total

    wait_bytes(send1.at[pl.ds(0, devices - 1)], sends.at[1])
    wait_bytes(recv2.at[pl.ds(0, devices - 1)], sends.at[2])
    wait_bytes(send3.at[pl.ds(0, n_map - 1)], sends.at[0])


def finish(packed, hess_out, grad_out, cost_out, lines):
    own_scans = grad_out.shape[1]
    total = packed[0:8, :]
    lined = [total] + [pltpu.roll(total, LANES - own_scans * c, 1) for c in range(1, 4)]

    def row_at(name):
        k = ROWS.index(name)
        return lined[k // 8][k % 8 : k % 8 + 1]

    lines[...] = jnp.zeros_like(lines)
    for i in range(6):
        for j in range(6):
            lines[6 * i + j : 6 * i + j + 1, :] = row_at(("h", min(i, j), max(i, j)))
        grad_out[i : i + 1, :] = row_at(("g", i))[:, 0:own_scans]
    hess_out[...] = lines[...].T[0:own_scans, 0:36]
    for h in range(cost_out.shape[1] // LANES):
        cost_out[:, h * LANES : (h + 1) * LANES] = packed[8 + h : 9 + h, :]


def local(points, poses, normal_angles, voxel_ids, scan_ids):
    blocks, npoints = points.shape[1:]
    n_tm, n_map = lax.axis_size("tm"), lax.axis_size("map")
    devices = n_tm * n_map
    slots = blocks // devices
    chunks = blocks // LANES
    vox_count = normal_angles.shape[1]
    own_scans = poses.shape[1]
    assert LANES % slots == 0 and own_scans * 4 == LANES and n_map % 4 == 0
    assert npoints == LANES and slots * 4 == LANES
    scale = own_scans * devices / (blocks * devices * npoints)
    f32 = jnp.float32
    vmem = pl.BlockSpec(memory_space=pltpu.VMEM)
    extra = -(-(vox_count // LANES) // 8) * 8
    packed = pl.pallas_call(
        functools.partial(kernel, (n_tm, n_map, slots, float(npoints), scale)),
        out_shape=jax.ShapeDtypeStruct((8 + extra, LANES), f32),
        in_specs=[pl.BlockSpec(memory_space=pl.ANY)] + [vmem] * 4,
        out_specs=vmem,
        scratch_shapes=[
            pltpu.VMEM(points.shape, f32),
            pltpu.VMEM((8, LANES), f32),
            pltpu.VMEM((chunks * 24, LANES), f32),
            pltpu.VMEM((chunks * 32, LANES), f32),
            pltpu.VMEM((chunks * 16, LANES), f32),
            pltpu.VMEM((8, vox_count), f32),
            pltpu.VMEM((devices, 6, LANES), f32),
            pltpu.VMEM((devices, 6, LANES), f32),
            pltpu.VMEM((chunks * 32, LANES), f32),
            pltpu.VMEM((devices, 1, LANES), f32),
            pltpu.VMEM((devices, 1, LANES), f32),
            pltpu.VMEM((devices, LANES), f32),
            pltpu.VMEM((chunks * 32, LANES), f32),
            pltpu.VMEM((n_map, 8, LANES), f32),
            pltpu.VMEM((n_map, 8, LANES), f32),
            pltpu.SemaphoreType.DMA((chunks,)),
            pltpu.SemaphoreType.DMA((3,)),
            pltpu.SemaphoreType.DMA((3,)),
        ],
        compiler_params=pltpu.CompilerParams(collective_id=0, has_side_effects=True),
    )(
        points,
        poses,
        normal_angles,
        voxel_ids.reshape(chunks, LANES),
        scan_ids.reshape(chunks, LANES),
    )
    hess, grad, cost = pl.pallas_call(
        finish,
        out_shape=(
            jax.ShapeDtypeStruct((own_scans, 36), f32),
            jax.ShapeDtypeStruct((6, own_scans), f32),
            jax.ShapeDtypeStruct((1, vox_count), f32),
        ),
        in_specs=[vmem],
        out_specs=(vmem, vmem, vmem),
        scratch_shapes=[pltpu.VMEM((LANES, LANES), f32)],
    )(packed)
    return hess.T, grad, cost.reshape(vox_count)


def solution(mesh):
    return jax.shard_map(
        local,
        mesh=mesh,
        in_specs=(
            P(None, ("tm", "map"), None),
            P(None, ("tm", "map")),
            P(None, ("tm", "map")),
            P(("tm", "map")),
            P(("tm", "map")),
        ),
        out_specs=(P(None, ("tm", "map")), P(None, ("tm", "map")), P(("tm", "map"))),
        check_vma=False,
    )
```
